768 devices in a mesh: gx: 16 (over y, x_lo), gy: 4 (over x_hi, core), gz: 12 (over z).
Axes of the slice: x: 4 (x_hi: 2, x_lo: 2; x = x_hi * 2 + x_lo), y: 8, z: 12, core: 2. Of those that a mesh axis runs over, the one named last changes fastest.
Arguments:
- flow_state: float32 [6, 64, 64, 1536], P(None, 'gx', 'gy', 'gz'), may hold values from -6 to 6
Outputs:
- new_vorticity: float32 [3, 64, 64, 1536], P(None, 'gx', 'gy', 'gz')
The draws below stay inside these ranges and needn't reach their ends.
All inputs are finite; a program needn't handle non-finite values.
Results may differ from the reference program's by a relative error of at most 0.0001.
Values sent between devices are 32-bit elements; how exact they have to be, the bound alone decides.
No kernel may reach another device: no remote copies, remote signals or barrier semaphores. Data moves between devices by JAX's collectives and lax.ppermute only.
A program may use at most 64 MiB of HBM per device.

```python
import jax
import jax.numpy as jnp
from jax import lax

NX = 64
NY = 64
NZ = 1536


def block_scale(rng, extent, cuts, smallest, top_value):
    loudness = 1.0
    for axis_at, shards_of in cuts:
        steps = jax.random.uniform(jax.random.fold_in(jax.random.fold_in(rng, 6), axis_at), (shards_of,), jnp.float32, smallest / len(cuts), top_value / len(cuts))
        loudness = loudness * jnp.repeat(jnp.exp(steps), extent[axis_at] // shards_of).reshape((-1,) + (1,) * (len(extent) - 1 - axis_at))
    return loudness


def gaussian(rng, extent, scale, reach, cuts=(), kind=jnp.bfloat16):
    result = scale * jax.random.normal(rng, extent, jnp.float32)
    if cuts:
        result = result * block_scale(rng, extent, cuts, -0.22, 0.18)
    return jnp.clip(result, -reach, reach).astype(kind)


def setup_inputs(seed: int = 0) -> dict:
    seeds = jax.random.split(jax.random.key(seed), 2)
    return {
        "flow_state": gaussian(seeds[0], (6, NX, NY, NZ), 1.0, 6.0, ((1, 16), (2, 4), (3, 12)), jnp.float32),
    }


def derivatives(values, dimension):
    minus_two = jnp.roll(values, 2, axis=dimension)
    minus_one = jnp.roll(values, 1, axis=dimension)
    plus_one = jnp.roll(values, -1, axis=dimension)
    plus_two = jnp.roll(values, -2, axis=dimension)
    gradient = (8.0 * (plus_one - minus_one) - (plus_two - minus_two)) / 12.0
    curvature = (16.0 * (plus_one + minus_one) - (plus_two + minus_two) - 30.0 * values) / 12.0
    return (gradient, curvature)

def reference(flow_state):
    vorticity = flow_state[0:3]
    velocity = flow_state[3:6]
    gradients = []
    laplace = jnp.zeros_like(vorticity)
    for dimension in range(3):
        gradient, unused = derivatives(velocity, dimension + 1)
        unused_grad, curvature = derivatives(vorticity, dimension + 1)
        gradients.append(gradient)
        laplace = laplace + curvature
    strain = jnp.zeros(vorticity.shape[1:], jnp.float32)
    for gradient in gradients:
        strain = strain + lax.optimization_barrier(jnp.sum(gradient * gradient, axis=0))
    peak = jnp.max(strain)
    step_size = 0.25 / jnp.maximum(1.0, jnp.sqrt(peak))
    stretch = jnp.zeros_like(vorticity)
    for dimension in range(3):
        stretch = stretch + vorticity[dimension:dimension + 1] * gradients[dimension]
    return vorticity + step_size * (stretch + 0.5 * laplace)
```

```python
import jax
import jax.numpy as jnp
from jax import lax
from jax.sharding import Mesh
from jax.sharding import PartitionSpec as P

GX = ("gx_0", "gx_1")
GY = ("gy_0", "gy_1")
LINE = ("gy_1", "gz")
PLANE = ("gx_0", "gx_1", "gy_0")


def extended(array, sides, width):
    for axis, dim in sides:
        count, length = (lax.axis_size(axis), array.shape[dim])
        up = [(i, (i + 1) % count) for i in range(count)]
        down = [(j, i) for i, j in up]
        last = lax.slice_in_dim(array, length - width, length, axis=dim)
        initial = lax.slice_in_dim(array, 0, width, axis=dim)
        before = lax.ppermute(last, axis, up)
        after = lax.ppermute(initial, axis, down)
        array = jnp.concatenate([before, array, after], axis=dim)
    return array


def peak_of(strain):
    lanes = jnp.max(strain, axis=(0, 1)).reshape(1, 1, -1)
    for axes in (LINE, PLANE):
        count = lax.axis_size(axes)
        sent = jnp.broadcast_to(lanes, (count,) + lanes.shape[1:])
        lanes = jnp.max(lax.all_to_all(sent, axes, 0, 0, tiled=True), axis=0, keepdims=True)
    return jnp.max(lanes)


def window(values, dimension, offset, length):
    return lax.slice_in_dim(values, offset, offset + length, axis=dimension)


def derivatives(padded, dimension, length):
    minus_two = window(padded, dimension, 0, length)
    minus_one = window(padded, dimension, 1, length)
    center = window(padded, dimension, 2, length)
    plus_one = window(padded, dimension, 3, length)
    plus_two = window(padded, dimension, 4, length)
    gradient = (8.0 * (plus_one[3:6] - minus_one[3:6]) - (plus_two[3:6] - minus_two[3:6])) / 12.0
    curvature = (
        16.0 * (plus_one[0:3] + minus_one[0:3])
        - (plus_two[0:3] + minus_two[0:3])
        - 30.0 * center[0:3]
    ) / 12.0
    return (gradient, curvature)


def on_device(flow_state):
    extent = flow_state.shape[1:]
    slabs = [
        extended(flow_state, ((GX, 1),), 2),
        extended(flow_state, ((GY, 2),), 2),
        extended(flow_state, (("gz", 3),), 2),
    ]
    vorticity = flow_state[0:3]
    gradients = []
    laplace = jnp.zeros_like(vorticity)
    for dimension in range(3):
        gradient, curvature = derivatives(slabs[dimension], dimension + 1, extent[dimension])
        gradients.append(gradient)
        laplace = laplace + curvature
    strain = jnp.zeros(extent, jnp.float32)
    for gradient in gradients:
        strain = strain + jnp.sum(gradient * gradient, axis=0)
    peak = peak_of(strain)
    step_size = 0.25 / jnp.maximum(1.0, jnp.sqrt(peak))
    stretch = jnp.zeros_like(vorticity)
    for dimension in range(3):
        stretch = stretch + vorticity[dimension : dimension + 1] * gradients[dimension]
    return vorticity + step_size * (stretch + 0.5 * laplace)


def solution(mesh):
    finer = Mesh(
        mesh.devices.reshape(8, 2, 2, 2, mesh.shape["gz"]), ("gx_0", "gx_1", "gy_0", "gy_1", "gz")
    )
    placed = (P(None, GX, GY, "gz"),)
    return jax.shard_map(
        on_device, mesh=finer, in_specs=placed, out_specs=P(None, GX, GY, "gz"), check_vma=False
    )
```

```python
import jax
import jax.numpy as jnp
from jax import lax
from jax.experimental import pallas as pl
from jax.experimental.pallas import tpu as pltpu
from jax.sharding import Mesh
from jax.sharding import PartitionSpec as P

GX = ("gx_0", "gx_1")
GY = ("gy_0", "gy_1")
PLANE = ("gx_0", "gx_1", "gy_0", "gy_1")


def call(body, *arrays, outs, scratch=()):
    vmem = pl.BlockSpec(memory_space=pltpu.VMEM)
    return pl.pallas_call(
        body,
        out_shape=[jax.ShapeDtypeStruct(shape, jnp.float32) for shape in outs],
        in_specs=[vmem] * len(arrays),
        out_specs=[vmem] * len(outs),
        scratch_shapes=[pltpu.VMEM(shape, jnp.float32) for shape in scratch],
        compiler_params=pltpu.CompilerParams(vmem_limit_bytes=16 * 1024 * 1024),
    )(*arrays)


def iota(shape, axis):
    return lax.broadcasted_iota(jnp.int32, shape, axis)


def first_difference(minus_two, minus_one, plus_one, plus_two):
    return (8.0 * (plus_one - minus_one) - (plus_two - minus_two)) * (1.0 / 12.0)


def second_difference(minus_two, minus_one, center, plus_one, plus_two):
    return (16.0 * (plus_one + minus_one) - (plus_two + minus_two) - 30.0 * center) * (1.0 / 12.0)


def pack_faces(state, far_x, far_y, near_x, near_y):
    depth, rows = state.shape[1:3]
    odd_x, odd_y = lax.axis_index("gx_1"), lax.axis_index("gy_1")
    near_x[...] = state[:, pl.ds((depth - 2) * (1 - odd_x), 2)]
    far_x[...] = state[:, pl.ds((depth - 2) * odd_x, 2)]
    low, high = (state[:, :, :2], state[:, :, rows - 2 :])
    near_y[...] = jnp.where(odd_y == 0, high, low)
    far_y[...] = jnp.where(odd_y == 0, low, high)


def local_terms(state, far_x, far_y, near_x, near_y, change, sent, tall, wide):
    depth, rows, lanes = state.shape[1:]
    odd_x, odd_y = lax.axis_index("gx_1"), lax.axis_index("gy_1")
    tall[:, 2 : depth + 2] = state[...]
    tall[:, pl.ds((depth + 2) * (1 - odd_x), 2)] = near_x[...]
    tall[:, pl.ds((depth + 2) * odd_x, 2)] = far_x[...]
    wide[:, :, 8 : rows + 8] = state[...]
    wide[:, :, 6:8] = jnp.where(odd_y == 0, far_y[...], near_y[...])
    wide[:, :, rows + 8 : rows + 10] = jnp.where(odd_y == 0, near_y[...], far_y[...])
    lane = iota((depth, rows, lanes), 2)
    inner = jnp.logical_and(lane >= 2, lane < lanes - 2)

    def along(component, dimension):
        center = state[component]
        if dimension == 0:
            near = [tall[component, k : k + depth] for k in (0, 1, 3, 4)]
        elif dimension == 1:
            near = [wide[component, :, 8 + k : 8 + k + rows] for k in (-2, -1, 1, 2)]
        else:
            near = [
                jnp.where(keep, pltpu.roll(center, shift % lanes, 2), 0.0)
                for shift, keep in ((2, lane >= 2), (1, lane >= 1), (-1, lane < lanes - 1), (-2, lane < lanes - 2))
            ]
        return near[0], near[1], center, near[2], near[3]

    partial = jnp.zeros((depth, rows, lanes), jnp.float32)
    last = partial
    for component in range(3):
        total = jnp.zeros((depth, rows, lanes), jnp.float32)
        laplace = total
        for dimension in range(3):
            a, b, _, d, e = along(3 + component, dimension)
            gradient = first_difference(a, b, d, e)
            if dimension == 2:
                last = last + gradient * gradient
            else:
                partial = partial + gradient * gradient
            total = total + state[dimension] * gradient
            laplace = laplace + second_difference(*along(component, dimension))
        change[component] = total + 0.5 * laplace
    strain = jnp.where(inner, partial + last, 0.0)
    highest = jnp.max(strain, axis=(0, 1)).reshape(1, lanes)
    highest = jnp.maximum(highest, pltpu.roll(highest, lanes // 2, 1))

    cells = depth * rows
    row, column = (iota((8, lanes), 0), iota((8, lanes), 1))

    def edge(block):
        turned = block.T
        return pltpu.roll(jnp.where(row < 4, turned[:8], turned[lanes - 8 :]), 4, 0)

    first = edge(state[3:5].reshape(2 * cells, lanes))
    second = edge(jnp.concatenate([state[5].reshape(cells, lanes), partial.reshape(cells, lanes)], axis=0))
    third = edge(state[0:2].reshape(2 * cells, lanes))
    fourth = edge(jnp.concatenate([state[2].reshape(cells, lanes), jnp.zeros((cells, lanes), jnp.float32)], axis=0))
    swirl = jnp.where(row < 4, pltpu.roll(third, 6, 0), pltpu.roll(fourth, 2, 0))
    swirl = jnp.where(jnp.logical_and(row >= 4, column >= lanes // 2), highest, swirl)
    for k in range(sent.shape[0]):
        sent[k, 0:8] = first
        sent[k, 8:16] = second
        sent[k, 16:24] = swirl


def line_peak(line, sent):
    count, _, lanes = line.shape
    row, column = (iota((count, 8, lanes), 1), iota((count, 8, lanes), 2))
    half = column < lanes // 2

    def joined(start):
        here = line[:, start : start + 8]
        following = jnp.concatenate([here[1:], here[:1]], axis=0)
        return jnp.where(row < 4, here, following)

    def gradient(values):
        return first_difference(*[pltpu.roll(values, shift, 1) for shift in (2, 1, 7, 6)])

    first, second = (joined(0), joined(8))
    one, two = (gradient(first), gradient(second))
    one, two = (one * one, jnp.where(half, two * two, second))
    strain = one + pltpu.roll(one, lanes // 2, 2) + (two + pltpu.roll(two, lanes // 2, 2))
    strain = jnp.where(jnp.logical_and(row >= 2, row < 6), strain, 0.0)
    inside = jnp.where(jnp.logical_or(half, row < 4), 0.0, line[:, 16:24])
    highest = jnp.max(jnp.maximum(strain, inside), axis=(0, 1)).reshape(1, lanes)
    sent[...] = jnp.broadcast_to(highest[None], sent.shape)


def finish(plane, line, change, state, out):
    count, _, lanes = line.shape
    depth, rows = state.shape[1:3]
    me = lax.axis_index("gz")
    lower, upper = (lax.rem(me + count - 1, count), lax.rem(me + 1, count))
    peak = jnp.max(plane[...], axis=0)
    peak = jnp.max(peak, axis=1, keepdims=True)
    step_size = 0.25 / jnp.maximum(1.0, jnp.sqrt(peak))

    row = iota((8, lanes), 0)
    half = iota((1, lanes), 1) < lanes // 2
    before, after, own = (line[lower], line[upper], line[me])

    def turned(values, low, high, spin):
        a6, a7 = (before[values + 2 : values + 3], before[values + 3 : values + 4])
        b0, b1 = (after[values + 4 : values + 5], after[values + 5 : values + 6])
        v6, v7 = (before[low : low + 1], before[low + 1 : low + 2])
        c0, c1 = (after[low + 2 : low + 3], after[low + 3 : low + 4])
        slopes = (a6 - 8.0 * a7, a7, -b0, 8.0 * b0 - b1)
        bends = (16.0 * v7 - v6, -v7, -c0, 16.0 * c0 - c1)
        fixes = [(spin[k] * slopes[k] + 0.5 * bends[k]) * (1.0 / 12.0) for k in range(4)]
        top = jnp.where(row == 0, fixes[0], jnp.where(row == 1, fixes[1], 0.0))
        bottom = jnp.where(row == 6, fixes[2], jnp.where(row == 7, fixes[3], 0.0))
        return jnp.concatenate([top, jnp.zeros((lanes - 16, lanes), jnp.float32), bottom], axis=0).T

    spin = [own[k : k + 1] for k in (22, 23, 20, 21)]
    spin = [jnp.where(half, s, pltpu.roll(s, lanes // 2, 1)) for s in spin]
    cells = depth * rows
    pair = turned(0, 16, 16, spin).reshape(2, depth, rows, lanes)
    single = turned(8, 20, 20, spin)[:cells].reshape(1, depth, rows, lanes)
    step = step_size.reshape(1, 1, 1)
    out[0:2] = state[0:2] + step * (change[0:2] + pair)
    out[2:3] = state[2:3] + step * (change[2:3] + single)


def on_device(state):
    depth, rows, lanes = state.shape[1:]
    count, around, turn = (lax.axis_size(GX), lax.axis_size("gz"), lax.axis_size(GY))
    face_x, face_y = ((6, 2, rows, lanes), (6, depth, 2, lanes))
    far_x, far_y, near_x, near_y = call(pack_faces, state, outs=[face_x, face_y, face_x, face_y])
    pairs_x = [(i, (i + 1 if i % 2 else i - 1) % count) for i in range(count)]
    pairs_y = [(i, (i + 1 if i % 2 else i - 1) % turn) for i in range(turn)]
    far_x = lax.ppermute(far_x, GX, pairs_x)
    far_y = lax.ppermute(far_y, GY, pairs_y)
    near_x = lax.ppermute(near_x, "gx_1", [(0, 1), (1, 0)])
    near_y = lax.ppermute(near_y, "gy_1", [(0, 1), (1, 0)])
    change, line = call(
        local_terms, state, far_x, far_y, near_x, near_y,
        outs=[(3, depth, rows, lanes), (around, 24, lanes)],
        scratch=[(6, depth + 4, rows, lanes), (6, depth, rows + 16, lanes)],
    )
    line = lax.all_to_all(line, "gz", 0, 0, tiled=True)
    (plane,) = call(line_peak, line, outs=[(lax.axis_size(PLANE), 1, lanes)])
    plane = lax.all_to_all(plane, PLANE, 0, 0, tiled=True)
    return call(finish, plane, line, change, state, outs=[(3, depth, rows, lanes)])[0]


def solution(mesh):
    finer = Mesh(
        mesh.devices.reshape(8, 2, 2, 2, mesh.shape["gz"]), ("gx_0", "gx_1", "gy_0", "gy_1", "gz")
    )
    placed = P(None, GX, GY, "gz")
    return jax.shard_map(
        on_device, mesh=finer, in_specs=(placed,), out_specs=placed, check_vma=False
    )
```

```python
import jax
import jax.numpy as jnp
from jax import lax
from jax.experimental import pallas as pl
from jax.experimental.pallas import tpu as pltpu
from jax.sharding import Mesh
from jax.sharding import PartitionSpec as P

GX = ("gx_0", "gx_1")
GY = ("gy_0", "gy_1")
FIRST_OF_LINE = 9
FIRST_OF_PLANE = 35
PLANE = ("gx_0", "gx_1", "gy_0", "gy_1")


def call(body, *arrays, outs, scratch=()):
    vmem = pl.BlockSpec(memory_space=pltpu.VMEM)
    return pl.pallas_call(
        body,
        out_shape=[jax.ShapeDtypeStruct(shape, jnp.float32) for shape in outs],
        in_specs=[vmem] * len(arrays),
        out_specs=[vmem] * len(outs),
        scratch_shapes=[pltpu.VMEM(shape, jnp.float32) for shape in scratch],
        compiler_params=pltpu.CompilerParams(vmem_limit_bytes=16 * 1024 * 1024),
    )(*arrays)


def iota(shape, axis):
    return lax.broadcasted_iota(jnp.int32, shape, axis)


def first_difference(minus_two, minus_one, plus_one, plus_two):
    return (8.0 * (plus_one - minus_one) - (plus_two - minus_two)) * (1.0 / 12.0)


def second_difference(minus_two, minus_one, center, plus_one, plus_two):
    return (16.0 * (plus_one + minus_one) - (plus_two + minus_two) - 30.0 * center) * (1.0 / 12.0)


def pack_faces(state, far_x, far_y, near_x, near_y):
    depth, rows = state.shape[1:3]
    odd_x, odd_y = lax.axis_index("gx_1"), lax.axis_index("gy_1")
    near_x[...] = state[:, pl.ds((depth - 2) * (1 - odd_x), 2)]
    far_x[...] = state[:, pl.ds((depth - 2) * odd_x, 2)]
    low, high = (state[:, :, :2], state[:, :, rows - 2 :])
    near_y[...] = jnp.where(odd_y == 0, high, low)
    far_y[...] = jnp.where(odd_y == 0, low, high)


def local_terms(state, far_x, far_y, near_x, near_y, change, sent, tall, wide):
    depth, rows, lanes = state.shape[1:]
    odd_x, odd_y = lax.axis_index("gx_1"), lax.axis_index("gy_1")
    tall[:, 2 : depth + 2] = state[...]
    tall[:, pl.ds((depth + 2) * (1 - odd_x), 2)] = near_x[...]
    tall[:, pl.ds((depth + 2) * odd_x, 2)] = far_x[...]
    wide[:, :, 8 : rows + 8] = state[...]
    wide[:, :, 6:8] = jnp.where(odd_y == 0, far_y[...], near_y[...])
    wide[:, :, rows + 8 : rows + 10] = jnp.where(odd_y == 0, near_y[...], far_y[...])
    lane = iota((depth, rows, lanes), 2)
    inner = jnp.logical_and(lane >= 2, lane < lanes - 2)

    def along(component, dimension):
        center = state[component]
        if dimension == 0:
            near = [tall[component, k : k + depth] for k in (0, 1, 3, 4)]
        elif dimension == 1:
            near = [wide[component, :, 8 + k : 8 + k + rows] for k in (-2, -1, 1, 2)]
        else:
            near = [
                jnp.where(keep, pltpu.roll(center, shift % lanes, 2), 0.0)
                for shift, keep in ((2, lane >= 2), (1, lane >= 1), (-1, lane < lanes - 1), (-2, lane < lanes - 2))
            ]
        return near[0], near[1], center, near[2], near[3]

    partial = jnp.zeros((depth, rows, lanes), jnp.float32)
    last = partial
    for component in range(3):
        total = jnp.zeros((depth, rows, lanes), jnp.float32)
        laplace = total
        for dimension in range(3):
            a, b, _, d, e = along(3 + component, dimension)
            gradient = first_difference(a, b, d, e)
            if dimension == 2:
                last = last + gradient * gradient
            else:
                partial = partial + gradient * gradient
            total = total + state[dimension] * gradient
            laplace = laplace + second_difference(*along(component, dimension))
        change[component] = total + 0.5 * laplace
    strain = jnp.where(inner, partial + last, 0.0)
    highest = jnp.max(strain, axis=(0, 1)).reshape(1, lanes)
    highest = jnp.maximum(highest, pltpu.roll(highest, lanes // 2, 1))

    cells = depth * rows
    row, column = (iota((8, lanes), 0), iota((8, lanes), 1))

    def edge(block):
        turned = block.T
        return pltpu.roll(jnp.where(row < 4, turned[:8], turned[lanes - 8 :]), 4, 0)

    first = edge(state[3:5].reshape(2 * cells, lanes))
    second = edge(jnp.concatenate([state[5].reshape(cells, lanes), partial.reshape(cells, lanes)], axis=0))
    third = edge(state[0:2].reshape(2 * cells, lanes))
    fourth = edge(jnp.concatenate([state[2].reshape(cells, lanes), jnp.zeros((cells, lanes), jnp.float32)], axis=0))
    swirl = jnp.where(row < 4, pltpu.roll(third, 6, 0), pltpu.roll(fourth, 2, 0))
    swirl = jnp.where(jnp.logical_and(row >= 4, column >= lanes // 2), highest, swirl)
    for k in range(sent.shape[0]):
        sent[k, 0:8] = first
        sent[k, 8:16] = second
        sent[k, 16:24] = swirl


def line_peak(line, sent):
    count, _, lanes = line.shape
    row, column = (iota((count, 8, lanes), 1), iota((count, 8, lanes), 2))
    half = column < lanes // 2

    def joined(start):
        here = line[:, start : start + 8]
        following = jnp.concatenate([here[1:], here[:1]], axis=0)
        return jnp.where(row < 4, here, following)

    def gradient(values):
        return first_difference(*[pltpu.roll(values, shift, 1) for shift in (2, 1, 7, 6)])

    first, second = (joined(0), joined(8))
    one, two = (gradient(first), gradient(second))
    one, two = (one * one, jnp.where(half, two * two, second))
    strain = one + pltpu.roll(one, lanes // 2, 2) + (two + pltpu.roll(two, lanes // 2, 2))
    strain = jnp.where(jnp.logical_and(row >= 2, row < 6), strain, 0.0)
    inside = jnp.where(jnp.logical_or(half, row < 4), 0.0, line[:, 16:24])
    highest = jnp.max(jnp.maximum(strain, inside), axis=(0, 1)).reshape(1, lanes)
    sent[...] = jnp.broadcast_to(highest[None], sent.shape)


def finish(plane, line, change, state, out):
    count, _, lanes = line.shape
    depth, rows = state.shape[1:3]
    me = lax.rem(lax.axis_index("gz") + count - FIRST_OF_LINE, count)
    lower, upper = (lax.rem(me + count - 1, count), lax.rem(me + 1, count))
    peak = jnp.max(plane[...], axis=0)
    peak = jnp.max(peak, axis=1, keepdims=True)
    step_size = 0.25 / jnp.maximum(1.0, jnp.sqrt(peak))

    row = iota((8, lanes), 0)
    half = iota((1, lanes), 1) < lanes // 2
    before, after, own = (line[lower], line[upper], line[me])

    def turned(values, low, high, spin):
        a6, a7 = (before[values + 2 : values + 3], before[values + 3 : values + 4])
        b0, b1 = (after[values + 4 : values + 5], after[values + 5 : values + 6])
        v6, v7 = (before[low : low + 1], before[low + 1 : low + 2])
        c0, c1 = (after[low + 2 : low + 3], after[low + 3 : low + 4])
        slopes = (a6 - 8.0 * a7, a7, -b0, 8.0 * b0 - b1)
        bends = (16.0 * v7 - v6, -v7, -c0, 16.0 * c0 - c1)
        fixes = [(spin[k] * slopes[k] + 0.5 * bends[k]) * (1.0 / 12.0) for k in range(4)]
        top = jnp.where(row == 0, fixes[0], jnp.where(row == 1, fixes[1], 0.0))
        bottom = jnp.where(row == 6, fixes[2], jnp.where(row == 7, fixes[3], 0.0))
        return jnp.concatenate([top, jnp.zeros((lanes - 16, lanes), jnp.float32), bottom], axis=0).T

    spin = [own[k : k + 1] for k in (22, 23, 20, 21)]
    spin = [jnp.where(half, s, pltpu.roll(s, lanes // 2, 1)) for s in spin]
    cells = depth * rows
    pair = turned(0, 16, 16, spin).reshape(2, depth, rows, lanes)
    single = turned(8, 20, 20, spin)[:cells].reshape(1, depth, rows, lanes)
    step = step_size.reshape(1, 1, 1)
    out[0:2] = state[0:2] + step * (change[0:2] + pair)
    out[2:3] = state[2:3] + step * (change[2:3] + single)


def turned_group(axes, first):
    count = lax.axis_size(axes)
    return [[(i + first) % count for i in range(count)]]


def on_device(state):
    depth, rows, lanes = state.shape[1:]
    count, around, turn = (lax.axis_size(GX), lax.axis_size("gz"), lax.axis_size(GY))
    face_x, face_y = ((6, 2, rows, lanes), (6, depth, 2, lanes))
    far_x, far_y, near_x, near_y = call(pack_faces, state, outs=[face_x, face_y, face_x, face_y])
    pairs_x = [(i, (i + 1 if i % 2 else i - 1) % count) for i in range(count)]
    pairs_y = [(i, (i + 1 if i % 2 else i - 1) % turn) for i in range(turn)]
    far_x = lax.ppermute(far_x, GX, pairs_x)
    far_y = lax.ppermute(far_y, GY, pairs_y)
    near_x = lax.ppermute(near_x, "gx_1", [(0, 1), (1, 0)])
    near_y = lax.ppermute(near_y, "gy_1", [(0, 1), (1, 0)])
    change, line = call(
        local_terms, state, far_x, far_y, near_x, near_y,
        outs=[(3, depth, rows, lanes), (around, 24, lanes)],
        scratch=[(6, depth + 4, rows, lanes), (6, depth, rows + 16, lanes)],
    )
    line = lax.all_to_all(line, "gz", 0, 0, axis_index_groups=turned_group("gz", FIRST_OF_LINE), tiled=True)
    (plane,) = call(line_peak, line, outs=[(lax.axis_size(PLANE), 1, lanes)])
    plane = lax.all_to_all(plane, PLANE, 0, 0, axis_index_groups=turned_group(PLANE, FIRST_OF_PLANE), tiled=True)
    return call(finish, plane, line, change, state, outs=[(3, depth, rows, lanes)])[0]


def solution(mesh):
    finer = Mesh(
        mesh.devices.reshape(8, 2, 2, 2, mesh.shape["gz"]), ("gx_0", "gx_1", "gy_0", "gy_1", "gz")
    )
    placed = P(None, GX, GY, "gz")
    return jax.shard_map(
        on_device, mesh=finer, in_specs=(placed,), out_specs=placed, check_vma=False
    )
```

```python
import jax
import jax.numpy as jnp
from jax import lax
from jax.experimental import pallas as pl
from jax.experimental.pallas import tpu as pltpu
from jax.sharding import Mesh
from jax.sharding import PartitionSpec as P

GX = ("gx_0", "gx_1")
GY = ("gy_0", "gy_1")
FIRST_OF_LINE = 9
FIRST_OF_PLANE = 35
SLOT = 18
PLANE = ("gx_0", "gx_1", "gy_0", "gy_1")


def call(body, *arrays, outs, scratch=()):
    vmem = pl.BlockSpec(memory_space=pltpu.VMEM)
    return pl.pallas_call(
        body,
        out_shape=[jax.ShapeDtypeStruct(shape, jnp.float32) for shape in outs],
        in_specs=[vmem] * len(arrays),
        out_specs=[vmem] * len(outs),
        scratch_shapes=[pltpu.VMEM(shape, jnp.float32) for shape in scratch],
        compiler_params=pltpu.CompilerParams(vmem_limit_bytes=16 * 1024 * 1024),
    )(*arrays)


def iota(shape, axis):
    return lax.broadcasted_iota(jnp.int32, shape, axis)


def first_difference(minus_two, minus_one, plus_one, plus_two):
    return (8.0 * (plus_one - minus_one) - (plus_two - minus_two)) * (1.0 / 12.0)


def second_difference(minus_two, minus_one, center, plus_one, plus_two):
    return (16.0 * (plus_one + minus_one) - (plus_two + minus_two) - 30.0 * center) * (1.0 / 12.0)


def place_in_line(count):
    return lax.rem(lax.axis_index("gz") + count - FIRST_OF_LINE, count)


def pack_faces(state, far_x, far_y, near_x, near_y):
    depth, rows = state.shape[1:3]
    odd_x, odd_y = lax.axis_index("gx_1"), lax.axis_index("gy_1")
    near_x[...] = state[:, pl.ds((depth - 2) * (1 - odd_x), 2)]
    far_x[...] = state[:, pl.ds((depth - 2) * odd_x, 2)]
    low, high = (state[:, :, :2], state[:, :, rows - 2 :])
    near_y[...] = jnp.where(odd_y == 0, high, low)
    far_y[...] = jnp.where(odd_y == 0, low, high)


def local_terms(state, far_x, far_y, near_x, near_y, change, sent, spin, tall, wide):
    depth, rows, lanes = state.shape[1:]
    odd_x, odd_y = lax.axis_index("gx_1"), lax.axis_index("gy_1")
    tall[:, 2 : depth + 2] = state[...]
    tall[:, pl.ds((depth + 2) * (1 - odd_x), 2)] = near_x[...]
    tall[:, pl.ds((depth + 2) * odd_x, 2)] = far_x[...]
    wide[:, :, 8 : rows + 8] = state[...]
    wide[:, :, 6:8] = jnp.where(odd_y == 0, far_y[...], near_y[...])
    wide[:, :, rows + 8 : rows + 10] = jnp.where(odd_y == 0, near_y[...], far_y[...])
    lane = iota((depth, rows, lanes), 2)
    inner = jnp.logical_and(lane >= 2, lane < lanes - 2)

    def along(component, dimension):
        center = state[component]
        if dimension == 0:
            near = [tall[component, k : k + depth] for k in (0, 1, 3, 4)]
        elif dimension == 1:
            near = [wide[component, :, 8 + k : 8 + k + rows] for k in (-2, -1, 1, 2)]
        else:
            near = [
                jnp.where(keep, pltpu.roll(center, shift % lanes, 2), 0.0)
                for shift, keep in ((2, lane >= 2), (1, lane >= 1), (-1, lane < lanes - 1), (-2, lane < lanes - 2))
            ]
        return near[0], near[1], center, near[2], near[3]

    partial = jnp.zeros((depth, rows, lanes), jnp.float32)
    last = partial
    for component in range(3):
        total = jnp.zeros((depth, rows, lanes), jnp.float32)
        laplace = total
        for dimension in range(3):
            a, b, _, d, e = along(3 + component, dimension)
            gradient = first_difference(a, b, d, e)
            if dimension == 2:
                last = last + gradient * gradient
            else:
                partial = partial + gradient * gradient
            total = total + state[dimension] * gradient
            laplace = laplace + second_difference(*along(component, dimension))
        change[component] = total + 0.5 * laplace
    strain = jnp.where(inner, partial + last, 0.0)
    highest = jnp.max(strain, axis=(0, 1)).reshape(1, lanes)
    highest = jnp.maximum(highest, pltpu.roll(highest, lanes // 2, 1))

    cells = depth * rows
    row, column = (iota((8, lanes), 0), iota((8, lanes), 1))

    def edge(block):
        turned = block.T
        return pltpu.roll(jnp.where(row < 4, turned[:8], turned[lanes - 8 :]), 4, 0)

    first = edge(state[3:5].reshape(2 * cells, lanes))
    second = edge(jnp.concatenate([state[5].reshape(cells, lanes), partial.reshape(cells, lanes)], axis=0))
    third = edge(state[0:2].reshape(2 * cells, lanes))
    fourth = edge(jnp.concatenate([state[2].reshape(cells, lanes), jnp.zeros((cells, lanes), jnp.float32)], axis=0))
    spin[...] = fourth
    count = sent.shape[0] // SLOT
    upper = lax.rem(place_in_line(count) + 1, count)
    outer = pltpu.roll(fourth, lanes // 2, 1)
    free = column >= lanes // 2
    second = jnp.where(jnp.logical_and(free, row == 6), highest, second)
    margin = jnp.logical_and(free, row < 2)
    rising = jnp.where(margin, pltpu.roll(outer, 6, 0), second)
    falling = jnp.where(margin, pltpu.roll(outer, 4, 0), second)
    third_rising, third_falling = (third[2:4], third[4:6])
    for k in range(count):
        up = upper == k
        sent[SLOT * k : SLOT * k + 8] = first
        sent[SLOT * k + 8 : SLOT * k + 16] = jnp.where(up, rising, falling)
        sent[SLOT * k + 16 : SLOT * k + 18] = jnp.where(up, third_rising, third_falling)


def line_peak(line, sent):
    count, lanes = (line.shape[0] // SLOT, line.shape[1])
    row, column = (iota((count, 8, lanes), 1), iota((count, 8, lanes), 2))
    half = column < lanes // 2

    def tiles(start):
        return jnp.stack([line[SLOT * k + start : SLOT * k + start + 8] for k in range(count)])

    def joined(here):
        following = jnp.concatenate([here[1:], here[:1]], axis=0)
        return jnp.where(row < 4, here, following)

    def gradient(values):
        return first_difference(*[pltpu.roll(values, shift, 1) for shift in (2, 1, 7, 6)])

    lower_half = tiles(8)
    first, second = (joined(tiles(0)), joined(lower_half))
    one, two = (gradient(first), gradient(second))
    one, two = (one * one, jnp.where(half, two * two, second))
    strain = one + pltpu.roll(one, lanes // 2, 2) + (two + pltpu.roll(two, lanes // 2, 2))
    strain = jnp.where(jnp.logical_and(row >= 2, row < 6), strain, 0.0)
    inside = jnp.where(jnp.logical_or(half, row != 6), 0.0, lower_half)
    highest = jnp.max(jnp.maximum(strain, inside), axis=(0, 1)).reshape(1, lanes)
    sent[...] = jnp.broadcast_to(highest[None], sent.shape)


def finish(plane, line, change, spin, state, out):
    count, lanes = (line.shape[0] // SLOT, line.shape[1])
    depth, rows = state.shape[1:3]
    me = place_in_line(count)
    lower, upper = (lax.rem(me + count - 1, count), lax.rem(me + 1, count))
    peak = jnp.max(plane[...], axis=0)
    peak = jnp.max(peak, axis=1, keepdims=True)
    step_size = 0.25 / jnp.maximum(1.0, jnp.sqrt(peak))

    row = iota((8, lanes), 0)
    half = iota((1, lanes), 1) < lanes // 2

    def received(device, index):
        return line[pl.ds(SLOT * device + index, 1), :]

    def turned(values, low, aside, whirl):
        a6, a7, b0, b1 = (
            received(device, values + k) for device, k in ((lower, 2), (lower, 3), (upper, 4), (upper, 5))
        )
        v6, v7, c0, c1 = (
            received(device, low + k) for device, k in ((lower, 0), (lower, 1), (upper, 0), (upper, 1))
        )
        if aside:
            v6, v7, c0, c1 = (pltpu.roll(v, lanes // 2, 1) for v in (v6, v7, c0, c1))
        slopes = (a6 - 8.0 * a7, a7, -b0, 8.0 * b0 - b1)
        bends = (16.0 * v7 - v6, -v7, -c0, 16.0 * c0 - c1)
        fixes = [(whirl[k] * slopes[k] + 0.5 * bends[k]) * (1.0 / 12.0) for k in range(4)]
        top = jnp.where(row == 0, fixes[0], jnp.where(row == 1, fixes[1], 0.0))
        bottom = jnp.where(row == 6, fixes[2], jnp.where(row == 7, fixes[3], 0.0))
        return jnp.concatenate([top, jnp.zeros((lanes - 16, lanes), jnp.float32), bottom], axis=0).T

    whirl = [spin[k : k + 1] for k in (4, 5, 2, 3)]
    whirl = [jnp.where(half, v, pltpu.roll(v, lanes // 2, 1)) for v in whirl]
    cells = depth * rows
    pair = turned(0, 16, False, whirl).reshape(2, depth, rows, lanes)
    single = turned(8, 8, True, whirl)[:cells].reshape(1, depth, rows, lanes)
    step = step_size.reshape(1, 1, 1)
    out[0:2] = state[0:2] + step * (change[0:2] + pair)
    out[2:3] = state[2:3] + step * (change[2:3] + single)


def turned_group(axes, first):
    count = lax.axis_size(axes)
    return [[(i + first) % count for i in range(count)]]


def on_device(state):
    depth, rows, lanes = state.shape[1:]
    count, around, turn = (lax.axis_size(GX), lax.axis_size("gz"), lax.axis_size(GY))
    face_x, face_y = ((6, 2, rows, lanes), (6, depth, 2, lanes))
    far_x, far_y, near_x, near_y = call(pack_faces, state, outs=[face_x, face_y, face_x, face_y])
    pairs_x = [(i, (i + 1 if i % 2 else i - 1) % count) for i in range(count)]
    pairs_y = [(i, (i + 1 if i % 2 else i - 1) % turn) for i in range(turn)]
    far_x = lax.ppermute(far_x, GX, pairs_x)
    far_y = lax.ppermute(far_y, GY, pairs_y)
    near_x = lax.ppermute(near_x, "gx_1", [(0, 1), (1, 0)])
    near_y = lax.ppermute(near_y, "gy_1", [(0, 1), (1, 0)])
    change, line, spin = call(
        local_terms, state, far_x, far_y, near_x, near_y,
        outs=[(3, depth, rows, lanes), (around * SLOT, lanes), (8, lanes)],
        scratch=[(6, depth + 4, rows, lanes), (6, depth, rows + 16, lanes)],
    )
    line = line.reshape(-1, 1, lanes)
    line = lax.all_to_all(line, "gz", 0, 0, axis_index_groups=turned_group("gz", FIRST_OF_LINE), tiled=True)
    line = line.reshape(-1, lanes)
    (plane,) = call(line_peak, line, outs=[(lax.axis_size(PLANE), 1, lanes)])
    plane = lax.all_to_all(plane, PLANE, 0, 0, axis_index_groups=turned_group(PLANE, FIRST_OF_PLANE), tiled=True)
    return call(finish, plane, line, change, spin, state, outs=[(3, depth, rows, lanes)])[0]


def solution(mesh):
    finer = Mesh(
        mesh.devices.reshape(8, 2, 2, 2, mesh.shape["gz"]), ("gx_0", "gx_1", "gy_0", "gy_1", "gz")
    )
    placed = P(None, GX, GY, "gz")
    return jax.shard_map(
        on_device, mesh=finer, in_specs=(placed,), out_specs=placed, check_vma=False
    )
```

```python
import jax
import jax.numpy as jnp
from jax import lax
from jax.experimental import pallas as pl
from jax.experimental.pallas import tpu as pltpu
from jax.sharding import Mesh
from jax.sharding import PartitionSpec as P

GX = ("gx_0", "gx_1")
GY = ("gy_0", "gy_1")
FIRST_OF_LINE = 9
FIRST_OF_PLANE = 35
SLOT = 18
PLANE = ("gx_0", "gx_1", "gy_0", "gy_1")


def call(body, *arrays, outs, scratch=()):
    vmem = pl.BlockSpec(memory_space=pltpu.VMEM)
    return pl.pallas_call(
        body,
        out_shape=[jax.ShapeDtypeStruct(shape, jnp.float32) for shape in outs],
        in_specs=[vmem] * len(arrays),
        out_specs=[vmem] * len(outs),
        scratch_shapes=[pltpu.VMEM(shape, jnp.float32) for shape in scratch],
        compiler_params=pltpu.CompilerParams(vmem_limit_bytes=16 * 1024 * 1024),
    )(*arrays)


def iota(shape, axis):
    return lax.broadcasted_iota(jnp.int32, shape, axis)


def first_difference(minus_two, minus_one, plus_one, plus_two):
    return (8.0 * (plus_one - minus_one) - (plus_two - minus_two)) * (1.0 / 12.0)


def second_difference(minus_two, minus_one, center, plus_one, plus_two):
    return (16.0 * (plus_one + minus_one) - (plus_two + minus_two) - 30.0 * center) * (1.0 / 12.0)


def place_in_line(count):
    return lax.rem(lax.axis_index("gz") + count - FIRST_OF_LINE, count)


def pack_faces(state, far_x, far_y, near_x, near_y):
    depth, rows = state.shape[1:3]
    odd_x, odd_y = lax.axis_index("gx_1"), lax.axis_index("gy_1")
    near_x[...] = state[:, pl.ds((depth - 2) * (1 - odd_x), 2)]
    far_x[...] = state[:, pl.ds((depth - 2) * odd_x, 2)]
    low, high = (state[:, :, :2], state[:, :, rows - 2 :])
    near_y[...] = jnp.where(odd_y == 0, high, low)
    far_y[...] = jnp.where(odd_y == 0, low, high)


def local_terms(state, far_x, far_y, near_x, near_y, change, sent, spin, tall, wide):
    depth, rows, lanes = state.shape[1:]
    odd_x, odd_y = lax.axis_index("gx_1"), lax.axis_index("gy_1")
    tall[:, 2 : depth + 2] = state[...]
    tall[:, pl.ds((depth + 2) * (1 - odd_x), 2)] = near_x[...]
    tall[:, pl.ds((depth + 2) * odd_x, 2)] = far_x[...]
    wide[:, :, 8 : rows + 8] = state[...]
    wide[:, :, 6:8] = jnp.where(odd_y == 0, far_y[...], near_y[...])
    wide[:, :, rows + 8 : rows + 10] = jnp.where(odd_y == 0, near_y[...], far_y[...])
    lane = iota((depth, rows, lanes), 2)
    inner = jnp.logical_and(lane >= 2, lane < lanes - 2)

    def along(component, dimension):
        center = state[component]
        if dimension == 0:
            near = [tall[component, k : k + depth] for k in (0, 1, 3, 4)]
        elif dimension == 1:
            near = [wide[component, :, 8 + k : 8 + k + rows] for k in (-2, -1, 1, 2)]
        else:
            near = [
                jnp.where(keep, pltpu.roll(center, shift % lanes, 2), 0.0)
                for shift, keep in ((2, lane >= 2), (1, lane >= 1), (-1, lane < lanes - 1), (-2, lane < lanes - 2))
            ]
        return near[0], near[1], center, near[2], near[3]

    partial = jnp.zeros((depth, rows, lanes), jnp.float32)
    last = partial
    for component in range(3):
        total = jnp.zeros((depth, rows, lanes), jnp.float32)
        laplace = total
        for dimension in range(3):
            a, b, _, d, e = along(3 + component, dimension)
            gradient = first_difference(a, b, d, e)
            if dimension == 2:
                last = last + gradient * gradient
            else:
                partial = partial + gradient * gradient
            total = total + state[dimension] * gradient
            laplace = laplace + second_difference(*along(component, dimension))
        change[component] = total + 0.5 * laplace
    strain = jnp.where(inner, partial + last, 0.0)
    highest = jnp.max(strain, axis=(0, 1)).reshape(1, lanes)
    highest = jnp.maximum(highest, pltpu.roll(highest, lanes // 2, 1))

    cells = depth * rows
    row, column = (iota((8, lanes), 0), iota((8, lanes), 1))

    def edge(block):
        turned = block.T
        return pltpu.roll(jnp.where(row < 4, turned[:8], turned[lanes - 8 :]), 4, 0)

    first = edge(state[3:5].reshape(2 * cells, lanes))
    second = edge(jnp.concatenate([state[5].reshape(cells, lanes), partial.reshape(cells, lanes)], axis=0))
    third = edge(state[0:2].reshape(2 * cells, lanes))
    fourth = edge(jnp.concatenate([state[2].reshape(cells, lanes), jnp.zeros((cells, lanes), jnp.float32)], axis=0))
    spin[...] = fourth
    count = sent.shape[0] // SLOT
    upper = lax.rem(place_in_line(count) + 1, count)
    outer = pltpu.roll(fourth, lanes // 2, 1)
    free = column >= lanes // 2
    second = jnp.where(jnp.logical_and(free, row == 6), highest, second)
    margin = jnp.logical_and(free, row < 2)
    rising = jnp.where(margin, pltpu.roll(outer, 6, 0), second)
    falling = jnp.where(margin, pltpu.roll(outer, 4, 0), second)
    third_rising, third_falling = (third[2:4], third[4:6])
    for k in range(count):
        up = upper == k
        sent[SLOT * k : SLOT * k + 8] = first
        sent[SLOT * k + 8 : SLOT * k + 16] = jnp.where(up, rising, falling)
        sent[SLOT * k + 16 : SLOT * k + 18] = jnp.where(up, third_rising, third_falling)


def line_peak(line, sent):
    count, lanes = (line.shape[0] // SLOT, line.shape[1])
    row, column = (iota((count, 8, lanes), 1), iota((count, 8, lanes), 2))
    half = column < lanes // 2

    def tiles(start):
        return jnp.stack([line[SLOT * k + start : SLOT * k + start + 8] for k in range(count)])

    def joined(here):
        following = jnp.concatenate([here[1:], here[:1]], axis=0)
        return jnp.where(row < 4, here, following)

    def gradient(values):
        return first_difference(*[pltpu.roll(values, shift, 1) for shift in (2, 1, 7, 6)])

    lower_half = tiles(8)
    first, second = (joined(tiles(0)), joined(lower_half))
    one, two = (gradient(first), gradient(second))
    one, two = (one * one, jnp.where(half, two * two, second))
    strain = one + pltpu.roll(one, lanes // 2, 2) + (two + pltpu.roll(two, lanes // 2, 2))
    strain = jnp.where(jnp.logical_and(row >= 2, row < 6), strain, 0.0)
    inside = jnp.where(jnp.logical_or(half, row != 6), 0.0, lower_half)
    highest = jnp.max(jnp.maximum(strain, inside), axis=(0, 1)).reshape(1, lanes)
    sent[...] = jnp.broadcast_to(highest, sent.shape)


def finish(plane, line, change, spin, state, out, built, sems):
    count, lanes = (line.shape[0] // SLOT, line.shape[1])
    depth, rows = state.shape[1:3]
    me = place_in_line(count)
    lower, upper = (lax.rem(me + count - 1, count), lax.rem(me + 1, count))
    peak = jnp.max(jnp.max(plane[...], axis=0, keepdims=True), axis=1, keepdims=True)
    step_size = 0.25 / jnp.maximum(1.0, jnp.sqrt(peak))

    row = iota((8, lanes), 0)
    half = iota((1, lanes), 1) < lanes // 2

    def received(device, index):
        return line[pl.ds(SLOT * device + index, 1), :]

    def turned(values, low, aside, whirl):
        a6, a7, b0, b1 = (
            received(device, values + k) for device, k in ((lower, 2), (lower, 3), (upper, 4), (upper, 5))
        )
        v6, v7, c0, c1 = (
            received(device, low + k) for device, k in ((lower, 0), (lower, 1), (upper, 0), (upper, 1))
        )
        if aside:
            v6, v7, c0, c1 = (pltpu.roll(v, lanes // 2, 1) for v in (v6, v7, c0, c1))
        slopes = (a6 - 8.0 * a7, a7, -b0, 8.0 * b0 - b1)
        bends = (16.0 * v7 - v6, -v7, -c0, 16.0 * c0 - c1)
        fixes = [(whirl[k] * slopes[k] + 0.5 * bends[k]) * (1.0 / 12.0) for k in range(4)]
        top = jnp.where(row == 0, fixes[0], jnp.where(row == 1, fixes[1], 0.0))
        bottom = jnp.where(row == 6, fixes[2], jnp.where(row == 7, fixes[3], 0.0))
        return jnp.concatenate([top, jnp.zeros((lanes - 16, lanes), jnp.float32), bottom], axis=0).T

    whirl = [spin[k : k + 1] for k in (4, 5, 2, 3)]
    whirl = [jnp.where(half, v, pltpu.roll(v, lanes // 2, 1)) for v in whirl]
    cells = depth * rows
    pair = turned(0, 16, False, whirl).reshape(2, depth, rows, lanes)
    single = turned(8, 8, True, whirl)[:cells].reshape(depth, rows, lanes)
    step = step_size.reshape(1, 1)
    copies = []
    for component, added in enumerate((pair[0], pair[1], single)):
        built[component] = state[component] + step * (change[component] + added)
        copies.append(pltpu.make_async_copy(built.at[component], out.at[component], sems.at[component]))
        copies[-1].start()
    for copy in copies:
        copy.wait()


def turned_group(axes, first):
    count = lax.axis_size(axes)
    return [[(i + first) % count for i in range(count)]]


def on_device(state):
    depth, rows, lanes = state.shape[1:]
    count, around, turn = (lax.axis_size(GX), lax.axis_size("gz"), lax.axis_size(GY))
    face_x, face_y = ((6, 2, rows, lanes), (6, depth, 2, lanes))
    far_x, far_y, near_x, near_y = call(pack_faces, state, outs=[face_x, face_y, face_x, face_y])
    pairs_x = [(i, (i + 1 if i % 2 else i - 1) % count) for i in range(count)]
    pairs_y = [(i, (i + 1 if i % 2 else i - 1) % turn) for i in range(turn)]
    far_x = lax.ppermute(far_x, GX, pairs_x)
    far_y = lax.ppermute(far_y, GY, pairs_y)
    near_x = lax.ppermute(near_x, "gx_1", [(0, 1), (1, 0)])
    near_y = lax.ppermute(near_y, "gy_1", [(0, 1), (1, 0)])
    change, line, spin = call(
        local_terms, state, far_x, far_y, near_x, near_y,
        outs=[(3, depth, rows, lanes), (around * SLOT, lanes), (8, lanes)],
        scratch=[(6, depth + 4, rows, lanes), (6, depth, rows + 16, lanes)],
    )
    line = line.reshape(-1, 1, lanes)
    line = lax.all_to_all(line, "gz", 0, 0, axis_index_groups=turned_group("gz", FIRST_OF_LINE), tiled=True)
    line = line.reshape(-1, lanes)
    (plane,) = call(line_peak, line, outs=[(lax.axis_size(PLANE), lanes)])
    plane = plane.reshape(-1, 1, lanes)
    plane = lax.all_to_all(plane, PLANE, 0, 0, axis_index_groups=turned_group(PLANE, FIRST_OF_PLANE), tiled=True)
    plane = plane.reshape(-1, lanes)
    vmem = pl.BlockSpec(memory_space=pltpu.VMEM)
    whole = (3, depth, rows, lanes)
    return pl.pallas_call(
        finish,
        out_shape=jax.ShapeDtypeStruct(whole, jnp.float32),
        in_specs=[vmem] * 5,
        out_specs=pl.BlockSpec(memory_space=pl.ANY),
        scratch_shapes=[pltpu.VMEM(whole, jnp.float32), pltpu.SemaphoreType.DMA((3,))],
        compiler_params=pltpu.CompilerParams(vmem_limit_bytes=16 * 1024 * 1024),
    )(plane, line, change, spin, state)


def solution(mesh):
    finer = Mesh(
        mesh.devices.reshape(8, 2, 2, 2, mesh.shape["gz"]), ("gx_0", "gx_1", "gy_0", "gy_1", "gz")
    )
    placed = P(None, GX, GY, "gz")
    return jax.shard_map(
        on_device, mesh=finer, in_specs=(placed,), out_specs=placed, check_vma=False
    )
```

```python
import jax
import jax.numpy as jnp
from jax import lax
from jax.experimental import pallas as pl
from jax.experimental.pallas import tpu as pltpu
from jax.sharding import Mesh
from jax.sharding import PartitionSpec as P

GX = ("gx_0", "gx_1")
GY = ("gy_0", "gy_1")
FIRST_OF_LINE = 9
FIRST_OF_PLANE = 35
SLOT = 18
PLANE = ("gx_0", "gx_1", "gy_0", "gy_1")


def call(body, *arrays, outs, scratch=()):
    vmem = pl.BlockSpec(memory_space=pltpu.VMEM)
    return pl.pallas_call(
        body,
        out_shape=[jax.ShapeDtypeStruct(shape, jnp.float32) for shape in outs],
        in_specs=[vmem] * len(arrays),
        out_specs=[vmem] * len(outs),
        scratch_shapes=[pltpu.VMEM(shape, jnp.float32) for shape in scratch],
        compiler_params=pltpu.CompilerParams(vmem_limit_bytes=16 * 1024 * 1024),
    )(*arrays)


def iota(shape, axis):
    return lax.broadcasted_iota(jnp.int32, shape, axis)


def first_difference(minus_two, minus_one, plus_one, plus_two):
    return (8.0 * (plus_one - minus_one) - (plus_two - minus_two)) * (1.0 / 12.0)


def second_difference(minus_two, minus_one, center, plus_one, plus_two):
    return (16.0 * (plus_one + minus_one) - (plus_two + minus_two) - 30.0 * center) * (1.0 / 12.0)


def place_in_line(count):
    return lax.rem(lax.axis_index("gz") + count - FIRST_OF_LINE, count)


def pack_faces(state, far_x, far_y, near_x, near_y):
    depth, rows = state.shape[1:3]
    odd_x, odd_y = lax.axis_index("gx_1"), lax.axis_index("gy_1")
    near_x[...] = state[:, pl.ds((depth - 2) * (1 - odd_x), 2)]
    far_x[...] = state[:, pl.ds((depth - 2) * odd_x, 2)]
    low, high = (state[:, :, :2], state[:, :, rows - 2 :])
    near_y[...] = jnp.where(odd_y == 0, high, low)
    far_y[...] = jnp.where(odd_y == 0, low, high)


def local_terms(state, far_x, far_y, near_x, near_y, sent, spin, tall, wide):
    depth, rows, lanes = state.shape[1:]
    odd_x, odd_y = lax.axis_index("gx_1"), lax.axis_index("gy_1")
    tall[:, 2 : depth + 2] = state[...]
    tall[:, pl.ds((depth + 2) * (1 - odd_x), 2)] = near_x[...]
    tall[:, pl.ds((depth + 2) * odd_x, 2)] = far_x[...]
    wide[:, :, 8 : rows + 8] = state[...]
    wide[:, :, 6:8] = jnp.where(odd_y == 0, far_y[...], near_y[...])
    wide[:, :, rows + 8 : rows + 10] = jnp.where(odd_y == 0, near_y[...], far_y[...])
    lane = iota((depth, rows, lanes), 2)
    inner = jnp.logical_and(lane >= 2, lane < lanes - 2)

    def along(component, dimension):
        center = state[component]
        if dimension == 0:
            near = [tall[component, k : k + depth] for k in (0, 1, 3, 4)]
        elif dimension == 1:
            near = [wide[component, :, 8 + k : 8 + k + rows] for k in (-2, -1, 1, 2)]
        else:
            near = [
                jnp.where(keep, pltpu.roll(center, shift % lanes, 2), 0.0)
                for shift, keep in ((2, lane >= 2), (1, lane >= 1), (-1, lane < lanes - 1), (-2, lane < lanes - 2))
            ]
        return near[0], near[1], center, near[2], near[3]

    partial = jnp.zeros((depth, rows, lanes), jnp.float32)
    last = partial
    for component in range(3):
        for dimension in range(3):
            a, b, _, d, e = along(3 + component, dimension)
            gradient = first_difference(a, b, d, e)
            if dimension == 2:
                last = last + gradient * gradient
            else:
                partial = partial + gradient * gradient
    strain = jnp.where(inner, partial + last, 0.0)
    highest = jnp.max(strain, axis=(0, 1)).reshape(1, lanes)
    highest = jnp.maximum(highest, pltpu.roll(highest, lanes // 2, 1))

    cells = depth * rows
    row, column = (iota((8, lanes), 0), iota((8, lanes), 1))

    def edge(block):
        turned = block.T
        return pltpu.roll(jnp.where(row < 4, turned[:8], turned[lanes - 8 :]), 4, 0)

    first = edge(state[3:5].reshape(2 * cells, lanes))
    second = edge(jnp.concatenate([state[5].reshape(cells, lanes), partial.reshape(cells, lanes)], axis=0))
    third = edge(state[0:2].reshape(2 * cells, lanes))
    fourth = edge(jnp.concatenate([state[2].reshape(cells, lanes), jnp.zeros((cells, lanes), jnp.float32)], axis=0))
    spin[...] = fourth
    count = sent.shape[0] // SLOT
    upper = lax.rem(place_in_line(count) + 1, count)
    outer = pltpu.roll(fourth, lanes // 2, 1)
    free = column >= lanes // 2
    second = jnp.where(jnp.logical_and(free, row == 6), highest, second)
    margin = jnp.logical_and(free, row < 2)
    rising = jnp.where(margin, pltpu.roll(outer, 6, 0), second)
    falling = jnp.where(margin, pltpu.roll(outer, 4, 0), second)
    third_rising, third_falling = (third[2:4], third[4:6])
    for k in range(count):
        up = upper == k
        sent[SLOT * k : SLOT * k + 8] = first
        sent[SLOT * k + 8 : SLOT * k + 16] = jnp.where(up, rising, falling)
        sent[SLOT * k + 16 : SLOT * k + 18] = jnp.where(up, third_rising, third_falling)


def local_change(state, far_x, far_y, near_x, near_y, change, tall, wide):
    depth, rows, lanes = state.shape[1:]
    odd_x, odd_y = lax.axis_index("gx_1"), lax.axis_index("gy_1")
    tall[:, 2 : depth + 2] = state[...]
    tall[:, pl.ds((depth + 2) * (1 - odd_x), 2)] = near_x[...]
    tall[:, pl.ds((depth + 2) * odd_x, 2)] = far_x[...]
    wide[:, :, 8 : rows + 8] = state[...]
    wide[:, :, 6:8] = jnp.where(odd_y == 0, far_y[...], near_y[...])
    wide[:, :, rows + 8 : rows + 10] = jnp.where(odd_y == 0, near_y[...], far_y[...])
    lane = iota((depth, rows, lanes), 2)

    def along(component, dimension):
        center = state[component]
        if dimension == 0:
            near = [tall[component, k : k + depth] for k in (0, 1, 3, 4)]
        elif dimension == 1:
            near = [wide[component, :, 8 + k : 8 + k + rows] for k in (-2, -1, 1, 2)]
        else:
            near = [
                jnp.where(keep, pltpu.roll(center, shift % lanes, 2), 0.0)
                for shift, keep in ((2, lane >= 2), (1, lane >= 1), (-1, lane < lanes - 1), (-2, lane < lanes - 2))
            ]
        return near[0], near[1], center, near[2], near[3]

    for component in range(3):
        total = jnp.zeros((depth, rows, lanes), jnp.float32)
        laplace = total
        for dimension in range(3):
            a, b, _, d, e = along(3 + component, dimension)
            gradient = first_difference(a, b, d, e)
            total = total + state[dimension] * gradient
            laplace = laplace + second_difference(*along(component, dimension))
        change[component] = total + 0.5 * laplace


def line_peak(line, sent):
    count, lanes = (line.shape[0] // SLOT, line.shape[1])
    row, column = (iota((count, 8, lanes), 1), iota((count, 8, lanes), 2))
    half = column < lanes // 2

    def tiles(start):
        return jnp.stack([line[SLOT * k + start : SLOT * k + start + 8] for k in range(count)])

    def joined(here):
        following = jnp.concatenate([here[1:], here[:1]], axis=0)
        return jnp.where(row < 4, here, following)

    def gradient(values):
        return first_difference(*[pltpu.roll(values, shift, 1) for shift in (2, 1, 7, 6)])

    lower_half = tiles(8)
    first, second = (joined(tiles(0)), joined(lower_half))
    one, two = (gradient(first), gradient(second))
    one, two = (one * one, jnp.where(half, two * two, second))
    strain = one + pltpu.roll(one, lanes // 2, 2) + (two + pltpu.roll(two, lanes // 2, 2))
    strain = jnp.where(jnp.logical_and(row >= 2, row < 6), strain, 0.0)
    inside = jnp.where(jnp.logical_or(half, row != 6), 0.0, lower_half)
    highest = jnp.max(jnp.maximum(strain, inside), axis=(0, 1)).reshape(1, lanes)
    sent[...] = jnp.broadcast_to(highest[None], sent.shape)


def finish(plane, line, change, spin, state, out):
    count, lanes = (line.shape[0] // SLOT, line.shape[1])
    depth, rows = state.shape[1:3]
    me = place_in_line(count)
    lower, upper = (lax.rem(me + count - 1, count), lax.rem(me + 1, count))
    peak = jnp.max(plane[...], axis=0)
    peak = jnp.max(peak, axis=1, keepdims=True)
    step_size = 0.25 / jnp.maximum(1.0, jnp.sqrt(peak))

    row = iota((8, lanes), 0)
    half = iota((1, lanes), 1) < lanes // 2

    def received(device, index):
        return line[pl.ds(SLOT * device + index, 1), :]

    def turned(values, low, aside, whirl):
        a6, a7, b0, b1 = (
            received(device, values + k) for device, k in ((lower, 2), (lower, 3), (upper, 4), (upper, 5))
        )
        v6, v7, c0, c1 = (
            received(device, low + k) for device, k in ((lower, 0), (lower, 1), (upper, 0), (upper, 1))
        )
        if aside:
            v6, v7, c0, c1 = (pltpu.roll(v, lanes // 2, 1) for v in (v6, v7, c0, c1))
        slopes = (a6 - 8.0 * a7, a7, -b0, 8.0 * b0 - b1)
        bends = (16.0 * v7 - v6, -v7, -c0, 16.0 * c0 - c1)
        fixes = [(whirl[k] * slopes[k] + 0.5 * bends[k]) * (1.0 / 12.0) for k in range(4)]
        top = jnp.where(row == 0, fixes[0], jnp.where(row == 1, fixes[1], 0.0))
        bottom = jnp.where(row == 6, fixes[2], jnp.where(row == 7, fixes[3], 0.0))
        return jnp.concatenate([top, jnp.zeros((lanes - 16, lanes), jnp.float32), bottom], axis=0).T

    whirl = [spin[k : k + 1] for k in (4, 5, 2, 3)]
    whirl = [jnp.where(half, v, pltpu.roll(v, lanes // 2, 1)) for v in whirl]
    cells = depth * rows
    pair = turned(0, 16, False, whirl).reshape(2, depth, rows, lanes)
    single = turned(8, 8, True, whirl)[:cells].reshape(1, depth, rows, lanes)
    step = step_size.reshape(1, 1, 1)
    out[0:2] = state[0:2] + step * (change[0:2] + pair)
    out[2:3] = state[2:3] + step * (change[2:3] + single)


def turned_group(axes, first):
    count = lax.axis_size(axes)
    return [[(i + first) % count for i in range(count)]]


def on_device(state):
    depth, rows, lanes = state.shape[1:]
    count, around, turn = (lax.axis_size(GX), lax.axis_size("gz"), lax.axis_size(GY))
    face_x, face_y = ((6, 2, rows, lanes), (6, depth, 2, lanes))
    far_x, far_y, near_x, near_y = call(pack_faces, state, outs=[face_x, face_y, face_x, face_y])
    pairs_x = [(i, (i + 1 if i % 2 else i - 1) % count) for i in range(count)]
    pairs_y = [(i, (i + 1 if i % 2 else i - 1) % turn) for i in range(turn)]
    far_x = lax.ppermute(far_x, GX, pairs_x)
    far_y = lax.ppermute(far_y, GY, pairs_y)
    near_x = lax.ppermute(near_x, "gx_1", [(0, 1), (1, 0)])
    near_y = lax.ppermute(near_y, "gy_1", [(0, 1), (1, 0)])
    line, spin = call(
        local_terms, state, far_x, far_y, near_x, near_y,
        outs=[(around * SLOT, lanes), (8, lanes)],
        scratch=[(6, depth + 4, rows, lanes), (6, depth, rows + 16, lanes)],
    )
    (change,) = call(
        local_change, state, far_x, far_y, near_x, near_y,
        outs=[(3, depth, rows, lanes)],
        scratch=[(6, depth + 4, rows, lanes), (6, depth, rows + 16, lanes)],
    )
    line = line.reshape(-1, 1, lanes)
    line = lax.all_to_all(line, "gz", 0, 0, axis_index_groups=turned_group("gz", FIRST_OF_LINE), tiled=True)
    line = line.reshape(-1, lanes)
    (plane,) = call(line_peak, line, outs=[(lax.axis_size(PLANE), 1, lanes)])
    plane = lax.all_to_all(plane, PLANE, 0, 0, axis_index_groups=turned_group(PLANE, FIRST_OF_PLANE), tiled=True)
    return call(finish, plane, line, change, spin, state, outs=[(3, depth, rows, lanes)])[0]


def solution(mesh):
    finer = Mesh(
        mesh.devices.reshape(8, 2, 2, 2, mesh.shape["gz"]), ("gx_0", "gx_1", "gy_0", "gy_1", "gz")
    )
    placed = P(None, GX, GY, "gz")
    return jax.shard_map(
        on_device, mesh=finer, in_specs=(placed,), out_specs=placed, check_vma=False
    )
```
